256 devices in a mesh: gx: 8 (over z), gy: 8 (over y, x_hi), gz: 4 (over x_lo, core).
Axes of the slice: x: 4 (x_hi: 2, x_lo: 2; x = x_hi * 2 + x_lo), y: 4, z: 8, core: 2. Of those that a mesh axis runs over, the one named last changes fastest.
Arguments:
- hidden_acts: bfloat16 [4, 8, 8, 256, 16384], P('gz', 'gy', 'gx'), may hold values from -6 to 6
- output_grad: bfloat16 [4, 8, 8, 256, 32], P('gz', 'gy', 'gx'), may hold values from -6 to 6
- weights: bfloat16 [4, 8, 8, 32, 16384], P('gz', 'gy', 'gx'), may hold values from -6 to 6
- momentum: bfloat16 [4, 8, 8, 32, 16384], P('gz', 'gy', 'gx'), may hold values from -48 to 48
- worker_of_slot: int32 [256], replicated, may hold values from 0 to 255, each once
- round_shift: int32 [8], replicated, may hold values from 0 to 7, as said below
Outputs:
- mixed: bfloat16 [8, 8, 4, 32, 16384], P('gx', 'gy', 'gz')
- new_momentum: bfloat16 [4, 8, 8, 32, 16384], P('gz', 'gy', 'gx')
The draws below stay inside these ranges and needn't reach their ends.
Inputs may be any that keep to these rules, and one draw needn't show every extreme that they name: `round_shift`: each entry is below log2 of 256, so offsets are powers of two below 256; some round has offset 256 / 2 and some round offset 1.
All inputs are finite; a program needn't handle non-finite values.
Results may differ from the reference program's by a relative error of at most 0.0081.
Values may be sent and summed in bfloat16 or wider, within the bound.
A program may use at most 64 MiB of HBM per device.

```python
import jax
import jax.numpy as jnp
from jax import lax

FF = 16384
ROWS = 32
TOK = 256
ROUNDS = 8
WORKERS = 256
N_GX = 8
N_GY = 8
N_GZ = 4


def draw_round_shift(key, part):
    levels = WORKERS.bit_length() - 1
    first_key = jax.random.fold_in(key, 11)
    second_key = jax.random.fold_in(key, 23)
    values = jax.random.randint(first_key, (ROUNDS,), 0, levels, dtype=jnp.int32)
    order = jax.random.permutation(second_key, ROUNDS)
    values = values.at[order[0]].set(jnp.int32(levels - 1))
    values = values.at[order[1]].set(jnp.int32(0))
    return values.astype(jnp.int32)


def shard_levels(rng, shape, split, least, top_value):
    def one(position, shards_of):
        heights = jax.random.uniform(jax.random.fold_in(jax.random.fold_in(rng, 6), position), (shards_of,), jnp.float32, least / len(split), top_value / len(split))
        return jnp.repeat(jnp.exp(heights), shape[position] // shards_of).reshape((-1,) + (1,) * (len(shape) - position - 1))

    level = one(*split[0])
    for cut in split[1:]:
        level = level * one(*cut)
    return level


def scatter_about(key, extent, deviation, most, cuts=(), kind=jnp.bfloat16):
    entries = deviation * jax.random.normal(key, extent, jnp.float32)
    if cuts:
        entries = entries * shard_levels(key, extent, cuts, -0.22, 0.18)
    return jnp.clip(entries, -most, most).astype(kind)


def setup_inputs(seed: int = 0) -> dict:
    seeds = jax.random.split(jax.random.key(seed), 7)
    return {
        "hidden_acts": scatter_about(seeds[0], (N_GZ, N_GY, N_GX, TOK, FF), 1.0, 6.0, ((0, 4), (1, 8), (2, 8))),
        "output_grad": scatter_about(seeds[1], (N_GZ, N_GY, N_GX, TOK, ROWS), 1.0, 6.0, ((0, 4), (1, 8), (2, 8))),
        "weights": scatter_about(seeds[2], (N_GZ, N_GY, N_GX, ROWS, FF), 1.0, 6.0, ((0, 4), (1, 8), (2, 8))),
        "momentum": scatter_about(seeds[3], (N_GZ, N_GY, N_GX, ROWS, FF), 8.0, 48.0, ((0, 4), (1, 8), (2, 8))),
        "worker_of_slot": jax.random.permutation(seeds[4], WORKERS).astype(jnp.int32),
        "round_shift": draw_round_shift(jax.random.fold_in(seeds[6], 71), 0),
    }


learn_rate = 0.01
beta_keep = 0.9


def local_step(items):
    hidden, grad_out, weight, moment = items
    grad = lax.dot_general(grad_out, hidden, (((0,), (0,)), ((), ())), preferred_element_type=jnp.float32)
    velocity = beta_keep * moment.astype(jnp.float32) + grad
    stepped = (weight.astype(jnp.float32) - learn_rate * velocity).astype(jnp.bfloat16)
    return stepped, velocity.astype(jnp.bfloat16)


def reference(hidden_acts, output_grad, weights, momentum, worker_of_slot, round_shift):
    workers = N_GX * N_GY * N_GZ
    hidden = hidden_acts.reshape(workers, TOK, FF)
    grad_out = output_grad.reshape(workers, TOK, ROWS)
    weight = weights.reshape(workers, ROWS, FF)
    moment = momentum.reshape(workers, ROWS, FF)
    stepped, new_moment = lax.map(local_step, (hidden, grad_out, weight, moment))
    replica = jnp.zeros_like(stepped).at[worker_of_slot].set(stepped)
    for step in range(ROUNDS):
        offset = jnp.left_shift(jnp.int32(1), round_shift[step].astype(jnp.int32))
        peer = jnp.roll(replica, offset, axis=0)
        replica = ((replica.astype(jnp.float32) + peer.astype(jnp.float32)) * 0.5).astype(jnp.bfloat16)
    mixed = replica.reshape(N_GX, N_GY, N_GZ, ROWS, FF)
    return mixed, new_moment.reshape(N_GZ, N_GY, N_GX, ROWS, FF)
```

```python
import jax
import jax.numpy as jnp
from jax import lax
from jax.sharding import PartitionSpec as P

ROUNDS = 8
learn_rate = 0.01
beta_keep = 0.9
AXES = ("gx", "gy", "gz")


def mixing(held, round_shift, workers):
    offsets = jnp.left_shift(jnp.int32(1), round_shift)
    half = ROUNDS // 2
    bits = (jnp.arange(1 << half)[:, None] >> jnp.arange(half)[None, :]) & 1
    low = jnp.sum(bits * offsets[:half][None, :], axis=1)
    high = jnp.sum(bits * offsets[half:][None, :], axis=1)
    index = jnp.arange(workers, dtype=jnp.int32)
    first = jnp.zeros((workers, workers), jnp.int32)
    second = jnp.zeros((workers, workers), jnp.int32)
    for m in range(1 << half):
        first += ((held[None, :] + low[m] - index[:, None]) & (workers - 1)) == 0
        second += ((index[None, :] + high[m] - index[:, None]) & (workers - 1)) == 0
    first = (first.astype(jnp.float32) / (1 << half)).astype(jnp.bfloat16)
    second = (second.astype(jnp.float32) / (1 << half)).astype(jnp.bfloat16)
    return jnp.dot(second, first, preferred_element_type=jnp.float32).astype(jnp.bfloat16)


def shards(hidden_acts, output_grad, weights, momentum, worker_of_slot, round_shift):
    hidden = hidden_acts.reshape(hidden_acts.shape[-2:])
    grad_out = output_grad.reshape(output_grad.shape[-2:])
    weight = weights.reshape(weights.shape[-2:])
    moment = momentum.reshape(momentum.shape[-2:])
    grad = lax.dot_general(
        grad_out, hidden, (((0,), (0,)), ((), ())), preferred_element_type=jnp.float32
    )
    velocity = beta_keep * moment.astype(jnp.float32) + grad
    new_moment = velocity.astype(jnp.bfloat16)
    stepped = (weight.astype(jnp.float32) - learn_rate * velocity).astype(jnp.bfloat16)
    count_x = lax.axis_size("gx")
    count_y = lax.axis_size("gy")
    count_z = lax.axis_size("gz")
    workers = count_x * count_y * count_z
    held = worker_of_slot.reshape(count_z, count_y, count_x).transpose(2, 1, 0).reshape(-1)
    mix = mixing(held, round_shift, workers)
    pieces = stepped.reshape(workers, -1)
    moved = lax.all_to_all(pieces, AXES, split_axis=0, concat_axis=0, tiled=True)
    mixed = jnp.dot(mix, moved, preferred_element_type=jnp.float32).astype(jnp.bfloat16)
    back = lax.all_to_all(mixed, AXES, split_axis=0, concat_axis=0, tiled=True)
    return (back.reshape(weights.shape), new_moment.reshape(momentum.shape))


def solution(mesh):
    placed = (
        P("gz", "gy", "gx", None, None),
        P("gz", "gy", "gx", None, None),
        P("gz", "gy", "gx", None, None),
        P("gz", "gy", "gx", None, None),
        P(),
        P(),
    )
    return jax.shard_map(
        shards,
        mesh=mesh,
        in_specs=placed,
        out_specs=(P("gx", "gy", "gz", None, None), P("gz", "gy", "gx", None, None)),
        check_vma=False,
    )
```

```python
import functools

import jax
import jax.numpy as jnp
from jax import lax
from jax.experimental import pallas as pl
from jax.experimental.pallas import tpu as pltpu
from jax.sharding import PartitionSpec as P

ROUNDS = 8
learn_rate = 0.01
beta_keep = 0.9
MESH = pl.DeviceIdType.MESH
TILE = (16, 128)


def zigzag(count):
    order = [0]
    for step in range(1, count // 2 + 1):
        order += sorted({step, count - step})
    return order


def kernel(
    sizes, grad_ref, hidden_hbm, weight_hbm, moment_hbm, source_ref, shift_ref,
    mixed_ref, moment_out,
    hidden, weight, moment, fresh, outgoing, arrived, ping, pong,
    in_sems, out_sems, send_sem, recv_sem, send_sem2, recv_sem2,
):
    nx, ny, nz = sizes
    devices = nx * ny * nz
    gx, gy, gz = (lax.axis_index(a) for a in ("gx", "gy", "gz"))
    me = (gx * ny + gy) * nz + gz
    cores, low_x = 2, nz // 2
    count_y, count_x = ny // 2, 2 * low_x
    core = lax.rem(gz, 2)
    x = lax.rem(gy, 2) * low_x + gz // 2
    y = gy // 2
    columns = count_x * count_y
    chunk = nx * TILE[1]

    def column_at(step):
        there_y = lax.rem(y + step // count_x, count_y)
        there_x = lax.rem(x + lax.rem(step, count_x), count_x)
        return there_y, there_x

    def device_at(there_y, there_x, there_gx, there_core):
        there_gy = there_y * 2 + there_x // low_x
        there_gz = lax.rem(there_x, low_x) * 2 + there_core
        return there_gx, there_gy, there_gz

    barrier = pltpu.get_barrier_semaphore()

    def greet(step, _):
        there_y, there_x = column_at(step)
        for dx in zigzag(nx):
            for dc in range(cores):
                target = device_at(there_y, there_x, lax.rem(gx + dx, nx), lax.rem(core + dc, 2))

                def signal():
                    pl.semaphore_signal(barrier, inc=1, device_id=target, device_id_type=MESH)

                if dx == 0 and dc == 0:
                    pl.when(step > 0)(signal)
                else:
                    signal()
        return 0

    def loads(step):
        there_y, there_x = column_at(step)
        at = pl.ds(pl.multiple_of((there_y * count_x + there_x) * chunk, chunk), chunk)
        return [
            pltpu.make_async_copy(big.at[:, at], small.at[:, at], in_sems.at[n, step])
            for n, (big, small) in enumerate(
                ((hidden_hbm, hidden), (weight_hbm, weight), (moment_hbm, moment))
            )
        ]

    def start_load(step, _):
        for copy in loads(step):
            copy.start()
        return 0

    lax.fori_loop(0, columns, start_load, 0)
    lax.fori_loop(0, columns, greet, 0)

    def tile_of(there_y, there_x, there_gx, there_core):
        return ((there_y * count_x + there_x) * nx + there_gx) * 2 + there_core

    my_tile = tile_of(y, x, gx, core)
    grad_out = grad_ref[...]

    def compute(step, _):
        there_y, there_x = column_at(step)
        base = pl.multiple_of((there_y * count_x + there_x) * chunk, chunk)
        at = pl.ds(base, chunk)
        for copy in loads(step):
            copy.wait()
        grad = jnp.dot(grad_out, hidden[:, at], preferred_element_type=jnp.float32)
        velocity = beta_keep * moment[:, at].astype(jnp.float32) + grad
        fresh[:, at] = velocity.astype(jnp.bfloat16)
        stepped = (weight[:, at].astype(jnp.float32) - learn_rate * velocity).astype(jnp.bfloat16)
        first = (there_y * count_x + there_x) * nx * 2
        for n in range(nx):
            for c in range(cores):
                outgoing[first + n * 2 + c] = stepped[
                    c * TILE[0] : (c + 1) * TILE[0], n * TILE[1] : (n + 1) * TILE[1]
                ]
        pltpu.make_async_copy(fresh.at[:, at], moment_out.at[:, at], out_sems.at[step]).start()

        @pl.when(step == 0)
        def _():
            pl.semaphore_wait(barrier, devices - 1)

        for dx in zigzag(nx):
            for dc in range(cores):
                there_gx, there_core = lax.rem(gx + dx, nx), lax.rem(core + dc, 2)
                target = device_at(there_y, there_x, there_gx, there_core)

                def send():
                    pltpu.make_async_remote_copy(
                        src_ref=outgoing.at[tile_of(there_y, there_x, there_gx, there_core)],
                        dst_ref=arrived.at[me],
                        send_sem=send_sem,
                        recv_sem=recv_sem,
                        device_id=target,
                        device_id_type=MESH,
                    ).start()

                if dx == 0 and dc == 0:
                    pl.when(step > 0)(send)
                else:
                    send()
        return 0

    lax.fori_loop(0, columns, compute, 0)
    arrived[me] = outgoing[my_tile]

    def all_of(ref, sem):
        piece = ref.at[pl.ds(0, devices - 1)]
        return pltpu.make_async_copy(piece, piece, sem)

    all_of(arrived, recv_sem).wait()

    group = 8
    mask = devices - 1
    first_off = jnp.left_shift(jnp.int32(1), shift_ref[0])

    def permute_and_mix(n, _):
        base = n * group
        for t in range(group):
            k = base + t
            one = arrived[source_ref[k]]
            two = arrived[source_ref[(k - first_off) & mask]]
            ping[k] = (one + two) * 0.5
        return 0

    lax.fori_loop(0, devices // group, permute_and_mix, 0)
    ping[pl.ds(devices, group)] = ping[pl.ds(0, group)]
    now, later = ping, pong
    for r in range(1, ROUNDS):
        off = jnp.left_shift(jnp.int32(1), shift_ref[r])

        def mix(n, _, now=now, later=later, off=off):
            base = n * group
            back = (base - off) & mask
            later[pl.ds(base, group)] = (now[pl.ds(base, group)] + now[pl.ds(back, group)]) * 0.5
            return 0

        lax.fori_loop(0, devices // group, mix, 0)
        if r < ROUNDS - 1:
            later[pl.ds(devices, group)] = later[pl.ds(0, group)]
        now, later = later, now
    done = now

    my_rows = pl.ds(pl.multiple_of(core * TILE[0], TILE[0]), TILE[0])
    my_lanes = pl.ds(pl.multiple_of(((y * count_x + x) * nx + gx) * TILE[1], TILE[1]), TILE[1])

    def give(step, _):
        there_y, there_x = column_at(step)
        for dx in zigzag(nx):
            for dc in range(cores):
                there_gx, there_core = lax.rem(gx + dx, nx), lax.rem(core + dc, 2)
                target = device_at(there_y, there_x, there_gx, there_core)
                worker = (target[0] * ny + target[1]) * nz + target[2]

                def send():
                    pltpu.make_async_remote_copy(
                        src_ref=done.at[worker],
                        dst_ref=mixed_ref.at[my_rows, my_lanes],
                        send_sem=send_sem2,
                        recv_sem=recv_sem2,
                        device_id=target,
                        device_id_type=MESH,
                    ).start()

                if dx == 0 and dc == 0:
                    pl.when(step > 0)(send)
                else:
                    send()
        return 0

    lax.fori_loop(0, columns, give, 0)
    mixed_ref[my_rows, my_lanes] = done[me]

    def drain(step, _):
        there_y, there_x = column_at(step)
        at = pl.ds(pl.multiple_of((there_y * count_x + there_x) * chunk, chunk), chunk)
        pltpu.make_async_copy(fresh.at[:, at], moment_out.at[:, at], out_sems.at[step]).wait()
        return 0

    lax.fori_loop(0, columns, drain, 0)
    all_of(arrived, send_sem).wait()
    all_of(arrived, send_sem2).wait()
    all_of(arrived, recv_sem2).wait()


def shards(sizes, hidden_acts, output_grad, weights, momentum, worker_of_slot, round_shift):
    nx, ny, nz = sizes
    devices = nx * ny * nz
    hidden = hidden_acts.reshape(hidden_acts.shape[-2:])
    grad_out = output_grad.reshape(output_grad.shape[-2:]).T
    weight = weights.reshape(weights.shape[-2:])
    moment = momentum.reshape(momentum.shape[-2:])
    rows, width = weight.shape
    slot = jnp.arange(devices, dtype=jnp.int32)
    place = (slot % nx * ny + slot // nx % ny) * nz + slot // (nx * ny)
    source = jnp.sum(
        jnp.where(worker_of_slot[None, :] == slot[:, None], place[None, :], 0), axis=1, dtype=jnp.int32
    )
    columns = devices // (2 * nx)
    tiles = (devices,) + TILE
    padded = (devices + 8,) + TILE
    vmem, smem, hbm = (
        pl.BlockSpec(memory_space=m) for m in (pltpu.VMEM, pltpu.SMEM, pltpu.HBM)
    )
    mixed, new_moment = pl.pallas_call(
        functools.partial(kernel, sizes),
        out_shape=[jax.ShapeDtypeStruct((rows, width), jnp.bfloat16)] * 2,
        in_specs=[vmem, hbm, hbm, hbm, smem, smem],
        out_specs=[vmem, hbm],
        scratch_shapes=[
            pltpu.VMEM(hidden.shape, jnp.bfloat16),
            pltpu.VMEM((rows, width), jnp.bfloat16),
            pltpu.VMEM((rows, width), jnp.bfloat16),
            pltpu.VMEM((rows, width), jnp.bfloat16),
            pltpu.VMEM(tiles, jnp.bfloat16),
            pltpu.VMEM(tiles, jnp.bfloat16),
            pltpu.VMEM(padded, jnp.bfloat16),
            pltpu.VMEM(padded, jnp.bfloat16),
            pltpu.SemaphoreType.DMA((3, columns)),
            pltpu.SemaphoreType.DMA((columns,)),
            pltpu.SemaphoreType.DMA,
            pltpu.SemaphoreType.DMA,
            pltpu.SemaphoreType.DMA,
            pltpu.SemaphoreType.DMA,
        ],
        compiler_params=pltpu.CompilerParams(
            collective_id=0, has_side_effects=True, vmem_limit_bytes=56 * 1024 * 1024
        ),
        name="step",
    )(grad_out, hidden, weight, moment, source, round_shift)
    return mixed.reshape(weights.shape), new_moment.reshape(momentum.shape)


def solution(mesh):
    sizes = tuple(mesh.shape[a] for a in ("gx", "gy", "gz"))
    placed = (
        P("gz", "gy", "gx", None, None),
        P("gz", "gy", "gx", None, None),
        P("gz", "gy", "gx", None, None),
        P("gz", "gy", "gx", None, None),
        P(),
        P(),
    )
    return jax.shard_map(
        functools.partial(shards, sizes),
        mesh=mesh,
        in_specs=placed,
        out_specs=(P("gx", "gy", "gz", None, None), P("gz", "gy", "gx", None, None)),
        check_vma=False,
    )
```

```python
import functools

import jax
import jax.numpy as jnp
from jax import lax
from jax.experimental import pallas as pl
from jax.experimental.pallas import tpu as pltpu
from jax.sharding import PartitionSpec as P

ROUNDS = 8
learn_rate = 0.01
beta_keep = 0.9
MESH = pl.DeviceIdType.MESH
TILE = (16, 128)


def zigzag(count):
    order = [0]
    for step in range(1, count // 2 + 1):
        order += sorted({step, count - step})
    return order


def kernel(
    sizes, grad_hbm, hidden_hbm, weight_hbm, moment_hbm, held_hbm, shift_hbm,
    mixed_ref, moment_out,
    hidden, weight, moment, outgoing, arrived, ping, pong, table, source_ref,
    grad_ref, held_ref, shift_ref, in_sems, table_sem, small_sems, send_sem, recv_sem, send_sem2, recv_sem2,
):
    nx, ny, nz = sizes
    devices = nx * ny * nz
    gx, gy, gz = (lax.axis_index(a) for a in ("gx", "gy", "gz"))
    me = (gx * ny + gy) * nz + gz
    cores, low_x = 2, nz // 2
    count_y, count_x = ny // 2, 2 * low_x
    core = lax.rem(gz, 2)
    x = lax.rem(gy, 2) * low_x + gz // 2
    y = gy // 2
    columns = count_x * count_y
    chunk = nx * TILE[1]

    def column_at(step):
        there_y = lax.rem(y + step // count_x, count_y)
        there_x = lax.rem(x + lax.rem(step, count_x), count_x)
        return there_y, there_x

    def device_at(there_y, there_x, there_gx, there_core):
        there_gy = there_y * 2 + there_x // low_x
        there_gz = lax.rem(there_x, low_x) * 2 + there_core
        return there_gx, there_gy, there_gz

    barrier = pltpu.get_barrier_semaphore()

    def greet(step, _):
        there_y, there_x = column_at(lax.rem(step + columns // 2, columns))
        for dx in reversed(zigzag(nx)):
            for dc in range(cores):
                target = device_at(there_y, there_x, lax.rem(gx + dx, nx), lax.rem(core + dc, 2))

                def signal():
                    pl.semaphore_signal(barrier, inc=1, device_id=target, device_id_type=MESH)

                if dx == 0 and dc == 0:
                    pl.when(step != columns // 2)(signal)
                else:
                    signal()
        return 0

    def loads(step):
        there_y, there_x = column_at(step)
        at = pl.ds(pl.multiple_of((there_y * count_x + there_x) * chunk, chunk), chunk)
        return [
            pltpu.make_async_copy(big.at[:, at], small.at[:, at], in_sems.at[n, step])
            for n, (big, small) in enumerate(
                ((hidden_hbm, hidden), (weight_hbm, weight), (moment_hbm, moment))
            )
        ]

    def start_load(step, _):
        for copy in loads(step):
            copy.start()
        return 0

    small_loads = [
        pltpu.make_async_copy(far, near, small_sems.at[n])
        for n, (far, near) in enumerate(
            ((grad_hbm, grad_ref), (held_hbm, held_ref), (shift_hbm, shift_ref))
        )
    ]
    for copy in small_loads:
        copy.start()
    start_load(0, 0)
    with jax.named_scope('s1_greet'):
        lax.fori_loop(0, columns, greet, 0)
    lax.fori_loop(1, columns, start_load, 0)

    def tile_of(there_y, there_x, there_gx, there_core):
        return ((there_y * count_x + there_x) * nx + there_gx) * 2 + there_core

    my_tile = tile_of(y, x, gx, core)
    for copy in small_loads:
        copy.wait()
    grad_out = grad_ref[...]

    def send_tiles(step, there_core):
        there_y, there_x = column_at(step)
        for dx in zigzag(nx):
            there_gx = lax.rem(gx + dx, nx)
            target = device_at(there_y, there_x, there_gx, there_core)

            def send():
                pltpu.make_async_remote_copy(
                    src_ref=outgoing.at[tile_of(there_y, there_x, there_gx, there_core)],
                    dst_ref=arrived.at[me],
                    send_sem=send_sem,
                    recv_sem=recv_sem,
                    device_id=target,
                    device_id_type=MESH,
                ).start()

            if dx == 0:
                pl.when((step > 0) | (core != there_core))(send)
            else:
                send()

    def compute(step, _):
        there_y, there_x = column_at(step)
        base = pl.multiple_of((there_y * count_x + there_x) * chunk, chunk)
        at = pl.ds(base, chunk)
        for copy in loads(step):
            copy.wait()
        grad = jnp.dot(grad_out, hidden[:, at], preferred_element_type=jnp.float32)
        velocity = beta_keep * moment[:, at].astype(jnp.float32) + grad
        moment_out[:, at] = velocity.astype(jnp.bfloat16)
        stepped = (weight[:, at].astype(jnp.float32) - learn_rate * velocity).astype(jnp.bfloat16)
        first = (there_y * count_x + there_x) * nx * 2
        for n in range(nx):
            for c in range(cores):
                outgoing[first + n * 2 + c] = stepped[
                    c * TILE[0] : (c + 1) * TILE[0], n * TILE[1] : (n + 1) * TILE[1]
                ]

        @pl.when(step == 0)
        def _():
            with jax.named_scope('s2_barrier'):
                pl.semaphore_wait(barrier, devices - 1)

        send_tiles(step, 0)
        return 0

    with jax.named_scope('s2_compute'):
        lax.fori_loop(0, columns, compute, 0)

    def second_wave(step, _):
        send_tiles(step, 1)
        return 0

    with jax.named_scope('s2_wave'):
        lax.fori_loop(0, columns, second_wave, 0)
    arrived[me] = outgoing[my_tile]

    held = jnp.broadcast_to(held_ref[...], (8, devices)).T[:, :1]
    slot = lax.broadcasted_iota(jnp.int32, (devices, devices), 0)
    worker = lax.broadcasted_iota(jnp.int32, (devices, devices), 1)
    place = (lax.rem(slot, nx) * ny + lax.rem(slot // nx, ny)) * nz + slot // (nx * ny)
    table[...] = jnp.sum(jnp.where(held == worker, place, 0), axis=0, keepdims=True) & (devices - 1)
    to_scalars = pltpu.make_async_copy(table, source_ref, table_sem)
    to_scalars.start()
    to_scalars.wait()

    def all_of(ref, sem):
        piece = ref.at[pl.ds(0, devices - 1)]
        return pltpu.make_async_copy(piece, piece, sem)

    with jax.named_scope('s3_recv1'):
        all_of(arrived, recv_sem).wait()

    group = 8
    wide = 16
    mask = devices - 1
    first_off = jnp.left_shift(jnp.int32(1), shift_ref[0])

    def permute_and_mix(n, _):
        base = n * group
        for t in range(group):
            k = base + t
            one = arrived[source_ref[0, k]]
            two = arrived[source_ref[0, (k - first_off) & mask]]
            ping[k] = (one + two) * 0.5
        return 0

    with jax.named_scope('s4_perm'):
        lax.fori_loop(0, devices // group, permute_and_mix, 0)
    ping[pl.ds(devices, group)] = ping[pl.ds(0, group)]
    now, later = ping, pong
    for r in range(1, ROUNDS):
        off = jnp.left_shift(jnp.int32(1), shift_ref[r])

        def mix(n, _, now=now, later=later, off=off):
            for part in range(wide // group):
                base = n * wide + part * group
                back = (base - off) & mask
                later[pl.ds(base, group)] = (
                    now[pl.ds(base, group)] + now[pl.ds(back, group)]
                ) * 0.5
            return 0

        with jax.named_scope('s5_mix'):
            lax.fori_loop(0, devices // wide, mix, 0)
        if r < ROUNDS - 1:
            later[pl.ds(devices, group)] = later[pl.ds(0, group)]
        now, later = later, now
    done = now

    my_rows = pl.ds(pl.multiple_of(core * TILE[0], TILE[0]), TILE[0])
    my_lanes = pl.ds(pl.multiple_of(((y * count_x + x) * nx + gx) * TILE[1], TILE[1]), TILE[1])

    def give(step, _):
        there_y, there_x = column_at(step)
        for dx in zigzag(nx):
            for dc in range(cores):
                there_gx, there_core = lax.rem(gx + dx, nx), lax.rem(core + dc, 2)
                target = device_at(there_y, there_x, there_gx, there_core)
                worker = (target[0] * ny + target[1]) * nz + target[2]

                def send():
                    pltpu.make_async_remote_copy(
                        src_ref=done.at[worker],
                        dst_ref=mixed_ref.at[my_rows, my_lanes],
                        send_sem=send_sem2,
                        recv_sem=recv_sem2,
                        device_id=target,
                        device_id_type=MESH,
                    ).start()

                if dx == 0 and dc == 0:
                    pl.when(step > 0)(send)
                else:
                    send()
        return 0

    with jax.named_scope('s6_give'):
        lax.fori_loop(0, columns, give, 0)
    mixed_ref[my_rows, my_lanes] = done[me]

    with jax.named_scope('s7_send1'):
        all_of(arrived, send_sem).wait()
    with jax.named_scope('s8_send2'):
        all_of(arrived, send_sem2).wait()
    with jax.named_scope('s9_recv2'):
        all_of(arrived, recv_sem2).wait()


def put_kernel(*refs):
    count = (len(refs) - 1) // 2
    sources, targets, sems = refs[:count], refs[count : 2 * count], refs[-1]
    parts = sems.shape[1]
    copies = []
    for n in range(count):
        width = sources[n].shape[1] // parts
        for p in range(parts):
            at = pl.ds(p * width, width)
            copies.append(
                pltpu.make_async_copy(sources[n].at[:, at], targets[n].at[:, at], sems.at[n, p])
            )
    for copy in copies:
        copy.start()
    for copy in copies:
        copy.wait()


def put(*arrays):
    parts = 4
    held = [pltpu.with_memory_space_constraint(a, pltpu.VMEM) for a in arrays]
    return pl.pallas_call(
        put_kernel,
        out_shape=[pltpu.HBM(a.shape, a.dtype) for a in arrays],
        in_specs=[pl.BlockSpec(memory_space=pltpu.VMEM)] * len(arrays),
        out_specs=[pl.BlockSpec(memory_space=pltpu.HBM)] * len(arrays),
        scratch_shapes=[pltpu.SemaphoreType.DMA((len(arrays), parts))],
        name="put",
    )(*held)


def shards(sizes, hidden_acts, output_grad, weights, momentum, worker_of_slot, round_shift):
    nx, ny, nz = sizes
    devices = nx * ny * nz
    hidden = hidden_acts.reshape(hidden_acts.shape[-2:])
    grad_out = output_grad.reshape(output_grad.shape[-2:]).T
    weight = weights.reshape(weights.shape[-2:])
    moment = momentum.reshape(momentum.shape[-2:])
    rows, width = weight.shape
    columns = devices // (2 * nx)
    tiles = (devices,) + TILE
    padded = (devices + 8,) + TILE
    inputs = [
        pltpu.with_memory_space_constraint(a, pltpu.HBM)
        for a in (grad_out, hidden, weight, moment, worker_of_slot.reshape(1, -1), round_shift)
    ]
    vmem, hbm = (pl.BlockSpec(memory_space=m) for m in (pltpu.VMEM, pltpu.HBM))
    mixed, new_moment = pl.pallas_call(
        functools.partial(kernel, sizes),
        out_shape=[pltpu.VMEM((rows, width), jnp.bfloat16)] * 2,
        in_specs=[hbm] * len(inputs),
        out_specs=[vmem, vmem],
        scratch_shapes=[
            pltpu.VMEM(hidden.shape, jnp.bfloat16),
            pltpu.VMEM((rows, width), jnp.bfloat16),
            pltpu.VMEM((rows, width), jnp.bfloat16),
            pltpu.VMEM(tiles, jnp.bfloat16),
            pltpu.VMEM(tiles, jnp.bfloat16),
            pltpu.VMEM(padded, jnp.bfloat16),
            pltpu.VMEM(padded, jnp.bfloat16),
            pltpu.VMEM((1, devices), jnp.int32),
            pltpu.SMEM((1, devices), jnp.int32),
            pltpu.VMEM(grad_out.shape, jnp.bfloat16),
            pltpu.VMEM((1, devices), jnp.int32),
            pltpu.SMEM((ROUNDS,), jnp.int32),
            pltpu.SemaphoreType.DMA((3, columns)),
            pltpu.SemaphoreType.DMA,
            pltpu.SemaphoreType.DMA((3,)),
            pltpu.SemaphoreType.DMA,
            pltpu.SemaphoreType.DMA,
            pltpu.SemaphoreType.DMA,
            pltpu.SemaphoreType.DMA,
        ],
        compiler_params=pltpu.CompilerParams(
            collective_id=0, has_side_effects=True, vmem_limit_bytes=40 * 1024 * 1024
        ),
        name="step",
    )(*inputs)
    mixed, new_moment = put(mixed, new_moment)
    return mixed.reshape(weights.shape), new_moment.reshape(momentum.shape)


def solution(mesh):
    sizes = tuple(mesh.shape[a] for a in ("gx", "gy", "gz"))
    placed = (
        P("gz", "gy", "gx", None, None),
        P("gz", "gy", "gx", None, None),
        P("gz", "gy", "gx", None, None),
        P("gz", "gy", "gx", None, None),
        P(),
        P(),
    )
    return jax.shard_map(
        functools.partial(shards, sizes),
        mesh=mesh,
        in_specs=placed,
        out_specs=(P("gx", "gy", "gz", None, None), P("gz", "gy", "gx", None, None)),
        check_vma=False,
    )
```

```python
import functools

import jax
import jax.numpy as jnp
from jax import lax
from jax.experimental import pallas as pl
from jax.experimental.pallas import tpu as pltpu
from jax.sharding import PartitionSpec as P

ROUNDS = 8
learn_rate = 0.01
beta_keep = 0.9
MESH = pl.DeviceIdType.MESH
TILE = (16, 128)


def zigzag(count):
    order = [0]
    for step in range(1, count // 2 + 1):
        order += sorted({step, count - step})
    return order


def kernel(
    sizes, grad_hbm, hidden_hbm, weight_hbm, moment_hbm, held_hbm, shift_hbm,
    mixed_ref, moment_out,
    hidden, weight, moment, outgoing, arrived, ping, pong, table, source_ref,
    grad_ref, held_ref, shift_ref, ready, in_sems, table_sem, small_sems, send_sem, recv_sem, send_sem2, recv_sem2,
):
    nx, ny, nz = sizes
    devices = nx * ny * nz
    gx, gy, gz = (lax.axis_index(a) for a in ("gx", "gy", "gz"))
    me = (gx * ny + gy) * nz + gz
    cores, low_x = 2, nz // 2
    count_y, count_x = ny // 2, 2 * low_x
    core = lax.rem(gz, 2)
    x = lax.rem(gy, 2) * low_x + gz // 2
    y = gy // 2
    columns = count_x * count_y
    chunk = nx * TILE[1]

    def column_at(step):
        there_y = lax.rem(y + step // count_x, count_y)
        there_x = lax.rem(x + lax.rem(step, count_x), count_x)
        return there_y, there_x

    def device_at(there_y, there_x, there_gx, there_core):
        there_gy = there_y * 2 + there_x // low_x
        there_gz = lax.rem(there_x, low_x) * 2 + there_core
        return there_gx, there_gy, there_gz

    barrier = pltpu.get_barrier_semaphore()

    def tell(semaphore, target):
        pl.semaphore_signal(semaphore, inc=1, device_id=target, device_id_type=MESH)

    def greet_plane(step, _):
        tell(barrier, device_at(*column_at(step), gx, core))
        return 0

    def greet():
        for dx in zigzag(nx):
            for dc in range(cores):
                if dx or dc:
                    tell(barrier, device_at(y, x, lax.rem(gx + dx, nx), lax.rem(core + dc, 2)))
        lax.fori_loop(1, columns, greet_plane, 0)

    def vouch(step, _):
        back_y = lax.rem(count_y - step // count_x, count_y)
        back_x = lax.rem(count_x - lax.rem(step, count_x), count_x)
        tell(ready.at[back_y * count_x + back_x], device_at(*column_at(step), gx, core))
        return 0

    def meet():
        pl.semaphore_wait(barrier, nx * cores - 1 + columns - 1)
        lax.fori_loop(1, columns, vouch, 0)

    def loads(step):
        there_y, there_x = column_at(step)
        at = pl.ds(pl.multiple_of((there_y * count_x + there_x) * chunk, chunk), chunk)
        return [
            pltpu.make_async_copy(big.at[:, at], small.at[:, at], in_sems.at[n, step])
            for n, (big, small) in enumerate(
                ((hidden_hbm, hidden), (weight_hbm, weight), (moment_hbm, moment))
            )
        ]

    def start_load(step, _):
        for copy in loads(step):
            copy.start()
        return 0

    small_loads = [
        pltpu.make_async_copy(far, near, small_sems.at[n])
        for n, (far, near) in enumerate(
            ((grad_hbm, grad_ref), (held_hbm, held_ref), (shift_hbm, shift_ref))
        )
    ]
    for copy in small_loads:
        copy.start()
    with jax.named_scope("s1_greet"):
        greet()
        lax.fori_loop(0, columns, start_load, 0)

    def tile_of(there_y, there_x, there_gx, there_core):
        return ((there_y * count_x + there_x) * nx + there_gx) * 2 + there_core

    my_tile = tile_of(y, x, gx, core)
    for copy in small_loads:
        copy.wait()
    grad_out = grad_ref[...]

    def send_tiles(step, there_core):
        there_y, there_x = column_at(step)
        for dx in zigzag(nx):
            there_gx = lax.rem(gx + dx, nx)
            target = device_at(there_y, there_x, there_gx, there_core)

            def send():
                pltpu.make_async_remote_copy(
                    src_ref=outgoing.at[tile_of(there_y, there_x, there_gx, there_core)],
                    dst_ref=arrived.at[me],
                    send_sem=send_sem,
                    recv_sem=recv_sem,
                    device_id=target,
                    device_id_type=MESH,
                ).start()

            if dx == 0:
                pl.when((step > 0) | (core != there_core))(send)
            else:
                send()

    def compute(step, _):
        there_y, there_x = column_at(step)
        base = pl.multiple_of((there_y * count_x + there_x) * chunk, chunk)
        at = pl.ds(base, chunk)
        for copy in loads(step):
            copy.wait()
        grad = jnp.dot(grad_out, hidden[:, at], preferred_element_type=jnp.float32)
        velocity = beta_keep * moment[:, at].astype(jnp.float32) + grad
        moment_out[:, at] = velocity.astype(jnp.bfloat16)
        stepped = (weight[:, at].astype(jnp.float32) - learn_rate * velocity).astype(jnp.bfloat16)
        first = (there_y * count_x + there_x) * nx * 2
        for n in range(nx):
            for c in range(cores):
                outgoing[first + n * 2 + c] = stepped[
                    c * TILE[0] : (c + 1) * TILE[0], n * TILE[1] : (n + 1) * TILE[1]
                ]

        @pl.when(step > 0)
        def _():
            pl.semaphore_wait(ready.at[step], 1)

        send_tiles(step, 0)
        return 0

    with jax.named_scope("s2_barrier"):
        meet()
    with jax.named_scope('s2_compute'):
        lax.fori_loop(0, columns, compute, 0)

    def second_wave(step, _):
        send_tiles(step, 1)
        return 0

    with jax.named_scope('s2_wave'):
        lax.fori_loop(0, columns, second_wave, 0)
    arrived[me] = outgoing[my_tile]

    held = jnp.broadcast_to(held_ref[...], (8, devices)).T[:, :1]
    slot = lax.broadcasted_iota(jnp.int32, (devices, devices), 0)
    worker = lax.broadcasted_iota(jnp.int32, (devices, devices), 1)
    place = (lax.rem(slot, nx) * ny + lax.rem(slot // nx, ny)) * nz + slot // (nx * ny)
    table[...] = jnp.sum(jnp.where(held == worker, place, 0), axis=0, keepdims=True) & (devices - 1)
    to_scalars = pltpu.make_async_copy(table, source_ref, table_sem)
    to_scalars.start()
    to_scalars.wait()

    def all_of(ref, sem):
        piece = ref.at[pl.ds(0, devices - 1)]
        return pltpu.make_async_copy(piece, piece, sem)

    with jax.named_scope('s3_recv1'):
        all_of(arrived, recv_sem).wait()

    group = 8
    wide = 16
    mask = devices - 1
    first_off = jnp.left_shift(jnp.int32(1), shift_ref[0])

    def permute_and_mix(n, _):
        base = n * group
        for t in range(group):
            k = base + t
            one = arrived[source_ref[0, k]]
            two = arrived[source_ref[0, (k - first_off) & mask]]
            ping[k] = (one + two) * 0.5
        return 0

    with jax.named_scope('s4_perm'):
        lax.fori_loop(0, devices // group, permute_and_mix, 0)
    ping[pl.ds(devices, group)] = ping[pl.ds(0, group)]
    now, later = ping, pong
    for r in range(1, ROUNDS):
        off = jnp.left_shift(jnp.int32(1), shift_ref[r])

        def mix(n, _, now=now, later=later, off=off):
            for part in range(wide // group):
                base = n * wide + part * group
                back = (base - off) & mask
                later[pl.ds(base, group)] = (
                    now[pl.ds(base, group)] + now[pl.ds(back, group)]
                ) * 0.5
            return 0

        with jax.named_scope('s5_mix'):
            lax.fori_loop(0, devices // wide, mix, 0)
        if r < ROUNDS - 1:
            later[pl.ds(devices, group)] = later[pl.ds(0, group)]
        now, later = later, now
    done = now

    my_rows = pl.ds(pl.multiple_of(core * TILE[0], TILE[0]), TILE[0])
    my_lanes = pl.ds(pl.multiple_of(((y * count_x + x) * nx + gx) * TILE[1], TILE[1]), TILE[1])

    def give(step, _):
        there_y, there_x = column_at(columns - 1 - step)
        for dx in reversed(zigzag(nx)):
            for dc in range(cores):
                there_gx, there_core = lax.rem(gx + dx, nx), lax.rem(core + dc, 2)
                target = device_at(there_y, there_x, there_gx, there_core)
                worker = (target[0] * ny + target[1]) * nz + target[2]

                def send():
                    pltpu.make_async_remote_copy(
                        src_ref=done.at[worker],
                        dst_ref=mixed_ref.at[my_rows, my_lanes],
                        send_sem=send_sem2,
                        recv_sem=recv_sem2,
                        device_id=target,
                        device_id_type=MESH,
                    ).start()

                if dx == 0 and dc == 0:
                    pl.when(step < columns - 1)(send)
                else:
                    send()
        return 0

    with jax.named_scope('s6_give'):
        lax.fori_loop(0, columns, give, 0)
    mixed_ref[my_rows, my_lanes] = done[me]

    with jax.named_scope('s7_send1'):
        all_of(arrived, send_sem).wait()
    with jax.named_scope('s8_send2'):
        all_of(arrived, send_sem2).wait()
    with jax.named_scope('s9_recv2'):
        all_of(arrived, recv_sem2).wait()


def put_kernel(*refs):
    count = (len(refs) - 1) // 2
    sources, targets, sems = refs[:count], refs[count : 2 * count], refs[-1]
    parts = sems.shape[1]
    copies = []
    for n in range(count):
        width = sources[n].shape[1] // parts
        for p in range(parts):
            at = pl.ds(p * width, width)
            copies.append(
                pltpu.make_async_copy(sources[n].at[:, at], targets[n].at[:, at], sems.at[n, p])
            )
    for copy in copies:
        copy.start()
    for copy in copies:
        copy.wait()


def put(*arrays):
    parts = 4
    held = [pltpu.with_memory_space_constraint(a, pltpu.VMEM) for a in arrays]
    return pl.pallas_call(
        put_kernel,
        out_shape=[pltpu.HBM(a.shape, a.dtype) for a in arrays],
        in_specs=[pl.BlockSpec(memory_space=pltpu.VMEM)] * len(arrays),
        out_specs=[pl.BlockSpec(memory_space=pltpu.HBM)] * len(arrays),
        scratch_shapes=[pltpu.SemaphoreType.DMA((len(arrays), parts))],
        name="put",
    )(*held)


def shards(sizes, hidden_acts, output_grad, weights, momentum, worker_of_slot, round_shift):
    nx, ny, nz = sizes
    devices = nx * ny * nz
    hidden = hidden_acts.reshape(hidden_acts.shape[-2:])
    grad_out = output_grad.reshape(output_grad.shape[-2:]).T
    weight = weights.reshape(weights.shape[-2:])
    moment = momentum.reshape(momentum.shape[-2:])
    rows, width = weight.shape
    columns = devices // (2 * nx)
    tiles = (devices,) + TILE
    padded = (devices + 8,) + TILE
    inputs = [
        pltpu.with_memory_space_constraint(a, pltpu.HBM)
        for a in (grad_out, hidden, weight, moment, worker_of_slot.reshape(1, -1), round_shift)
    ]
    vmem, hbm = (pl.BlockSpec(memory_space=m) for m in (pltpu.VMEM, pltpu.HBM))
    mixed, new_moment = pl.pallas_call(
        functools.partial(kernel, sizes),
        out_shape=[pltpu.VMEM((rows, width), jnp.bfloat16)] * 2,
        in_specs=[hbm] * len(inputs),
        out_specs=[vmem, vmem],
        scratch_shapes=[
            pltpu.VMEM(hidden.shape, jnp.bfloat16),
            pltpu.VMEM((rows, width), jnp.bfloat16),
            pltpu.VMEM((rows, width), jnp.bfloat16),
            pltpu.VMEM(tiles, jnp.bfloat16),
            pltpu.VMEM(tiles, jnp.bfloat16),
            pltpu.VMEM(padded, jnp.bfloat16),
            pltpu.VMEM(padded, jnp.bfloat16),
            pltpu.VMEM((1, devices), jnp.int32),
            pltpu.SMEM((1, devices), jnp.int32),
            pltpu.VMEM(grad_out.shape, jnp.bfloat16),
            pltpu.VMEM((1, devices), jnp.int32),
            pltpu.SMEM((ROUNDS,), jnp.int32),
            pltpu.SemaphoreType.REGULAR((columns,)),
            pltpu.SemaphoreType.DMA((3, columns)),
            pltpu.SemaphoreType.DMA,
            pltpu.SemaphoreType.DMA((3,)),
            pltpu.SemaphoreType.DMA,
            pltpu.SemaphoreType.DMA,
            pltpu.SemaphoreType.DMA,
            pltpu.SemaphoreType.DMA,
        ],
        compiler_params=pltpu.CompilerParams(
            collective_id=0, has_side_effects=True, vmem_limit_bytes=40 * 1024 * 1024
        ),
        name="step",
    )(*inputs)
    mixed, new_moment = put(mixed, new_moment)
    return mixed.reshape(weights.shape), new_moment.reshape(momentum.shape)


def solution(mesh):
    sizes = tuple(mesh.shape[a] for a in ("gx", "gy", "gz"))
    placed = (
        P("gz", "gy", "gx", None, None),
        P("gz", "gy", "gx", None, None),
        P("gz", "gy", "gx", None, None),
        P("gz", "gy", "gx", None, None),
        P(),
        P(),
    )
    return jax.shard_map(
        functools.partial(shards, sizes),
        mesh=mesh,
        in_specs=placed,
        out_specs=(P("gx", "gy", "gz", None, None), P("gz", "gy", "gx", None, None)),
        check_vma=False,
    )
```

```python
import functools

import jax
import jax.numpy as jnp
from jax import lax
from jax.experimental import pallas as pl
from jax.experimental.pallas import tpu as pltpu
from jax.sharding import PartitionSpec as P

ROUNDS = 8
learn_rate = 0.01
beta_keep = 0.9
MESH = pl.DeviceIdType.MESH
TILE = (16, 128)


def zigzag(count):
    order = [0]
    for step in range(1, count // 2 + 1):
        order += sorted({step, count - step})
    return order


def kernel(
    sizes, grad_hbm, hidden_hbm, weight_hbm, moment_hbm, held_hbm, shift_hbm,
    mixed_ref, moment_out,
    hidden, weight, moment, outgoing, arrived, ping, pong, table, source_ref,
    grad_ref, held_ref, shift_ref, ready, in_sems, table_sem, small_sems, send_sem, recv_sem, send_sem2, recv_sem2,
):
    nx, ny, nz = sizes
    devices = nx * ny * nz
    gx, gy, gz = (lax.axis_index(a) for a in ("gx", "gy", "gz"))
    me = (gx * ny + gy) * nz + gz
    cores, low_x = 2, nz // 2
    count_y, count_x = ny // 2, 2 * low_x
    core = lax.rem(gz, 2)
    x = lax.rem(gy, 2) * low_x + gz // 2
    y = gy // 2
    columns = count_x * count_y
    chunk = nx * TILE[1]

    def spread(turn):
        along_y = turn * count_x
        along_x = turn - (count_y - 1)
        rest = turn - (count_y + count_x - 1)
        others = (1 + rest // (count_x - 1)) * count_x + 1 + lax.rem(rest, count_x - 1)
        return jnp.where(
            turn < count_y, along_y, jnp.where(turn < count_y + count_x - 1, along_x, others)
        )

    def column_at(step):
        there_y = lax.rem(y + step // count_x, count_y)
        there_x = lax.rem(x + lax.rem(step, count_x), count_x)
        return there_y, there_x

    def device_at(there_y, there_x, there_gx, there_core):
        there_gy = there_y * 2 + there_x // low_x
        there_gz = lax.rem(there_x, low_x) * 2 + there_core
        return there_gx, there_gy, there_gz

    barrier = pltpu.get_barrier_semaphore()

    def tell(semaphore, target):
        pl.semaphore_signal(semaphore, inc=1, device_id=target, device_id_type=MESH)

    def peer(dy, dx):
        return device_at(lax.rem(y + dy, count_y), lax.rem(x + dx, count_x), gx, core)

    def greet():
        for dx in zigzag(nx):
            for dc in range(cores):
                if dx or dc:
                    tell(barrier, device_at(y, x, lax.rem(gx + dx, nx), lax.rem(core + dc, 2)))
        for dy in range(1, count_y):
            tell(barrier, peer(dy, 0))
        for dx in range(1, count_x):
            tell(barrier, peer(0, dx))

    def vouch_to(dy, dx, about_y):
        seen_y = (count_y - dy + about_y) % count_y
        tell(ready.at[seen_y * count_x + (count_x - dx) % count_x], peer(dy, dx))

    def meet():
        pl.semaphore_wait(barrier, nx * cores - 1 + count_y - 1 + count_x - 1)
        for dy in range(1, count_y):
            vouch_to(dy, 0, 0)
        for dx in range(1, count_x):
            vouch_to(0, dx, 0)

    def await_column(step):
        pl.semaphore_wait(ready.at[step], 1)
        for dy in range(1, count_y):

            @pl.when(step == dy * count_x)
            def _():
                for dx in range(1, count_x):
                    vouch_to(0, dx, dy)

    def loads(step):
        there_y, there_x = column_at(step)
        at = pl.ds(pl.multiple_of((there_y * count_x + there_x) * chunk, chunk), chunk)
        return [
            pltpu.make_async_copy(big.at[:, at], small.at[:, at], in_sems.at[n, step])
            for n, (big, small) in enumerate(
                ((hidden_hbm, hidden), (weight_hbm, weight), (moment_hbm, moment))
            )
        ]

    def start_load(turn, _):
        for copy in loads(spread(turn)):
            copy.start()
        return 0

    small_loads = [
        pltpu.make_async_copy(far, near, small_sems.at[n])
        for n, (far, near) in enumerate(
            ((grad_hbm, grad_ref), (held_hbm, held_ref), (shift_hbm, shift_ref))
        )
    ]
    for copy in small_loads:
        copy.start()
    with jax.named_scope("s1_greet"):
        greet()
        lax.fori_loop(0, columns, start_load, 0)

    def tile_of(there_y, there_x, there_gx, there_core):
        return ((there_y * count_x + there_x) * nx + there_gx) * 2 + there_core

    my_tile = tile_of(y, x, gx, core)
    for copy in small_loads:
        copy.wait()
    grad_out = grad_ref[...]

    def send_tiles(step, there_core):
        there_y, there_x = column_at(step)
        for dx in zigzag(nx):
            there_gx = lax.rem(gx + dx, nx)
            target = device_at(there_y, there_x, there_gx, there_core)

            def send():
                pltpu.make_async_remote_copy(
                    src_ref=outgoing.at[tile_of(there_y, there_x, there_gx, there_core)],
                    dst_ref=arrived.at[me],
                    send_sem=send_sem,
                    recv_sem=recv_sem,
                    device_id=target,
                    device_id_type=MESH,
                ).start()

            if dx == 0:
                pl.when((step > 0) | (core != there_core))(send)
            else:
                send()

    def compute(turn, _):
        step = spread(turn)
        there_y, there_x = column_at(step)
        base = pl.multiple_of((there_y * count_x + there_x) * chunk, chunk)
        at = pl.ds(base, chunk)
        for copy in loads(step):
            copy.wait()
        grad = jnp.dot(grad_out, hidden[:, at], preferred_element_type=jnp.float32)
        velocity = beta_keep * moment[:, at].astype(jnp.float32) + grad
        moment_out[:, at] = velocity.astype(jnp.bfloat16)
        stepped = (weight[:, at].astype(jnp.float32) - learn_rate * velocity).astype(jnp.bfloat16)
        first = (there_y * count_x + there_x) * nx * 2
        for n in range(nx):
            for c in range(cores):
                outgoing[first + n * 2 + c] = stepped[
                    c * TILE[0] : (c + 1) * TILE[0], n * TILE[1] : (n + 1) * TILE[1]
                ]

        @pl.when(step > 0)
        def _():
            await_column(step)

        send_tiles(step, 0)
        return 0

    with jax.named_scope("s2_barrier"):
        meet()
    with jax.named_scope('s2_compute'):
        lax.fori_loop(0, columns, compute, 0)

    def second_wave(step, _):
        send_tiles(step, 1)
        return 0

    with jax.named_scope('s2_wave'):
        lax.fori_loop(0, columns, second_wave, 0)
    arrived[me] = outgoing[my_tile]

    held = jnp.broadcast_to(held_ref[...], (8, devices)).T[:, :1]
    slot = lax.broadcasted_iota(jnp.int32, (devices, devices), 0)
    worker = lax.broadcasted_iota(jnp.int32, (devices, devices), 1)
    place = (lax.rem(slot, nx) * ny + lax.rem(slot // nx, ny)) * nz + slot // (nx * ny)
    table[...] = jnp.sum(jnp.where(held == worker, place, 0), axis=0, keepdims=True) & (devices - 1)
    to_scalars = pltpu.make_async_copy(table, source_ref, table_sem)
    to_scalars.start()
    to_scalars.wait()

    def all_of(ref, sem):
        piece = ref.at[pl.ds(0, devices - 1)]
        return pltpu.make_async_copy(piece, piece, sem)

    with jax.named_scope('s3_recv1'):
        all_of(arrived, recv_sem).wait()

    group = 8
    wide = 16
    mask = devices - 1
    first_off = jnp.left_shift(jnp.int32(1), shift_ref[0])

    def permute_and_mix(n, _):
        base = n * group
        for t in range(group):
            k = base + t
            one = arrived[source_ref[0, k]]
            two = arrived[source_ref[0, (k - first_off) & mask]]
            ping[k] = (one + two) * 0.5
        return 0

    with jax.named_scope('s4_perm'):
        lax.fori_loop(0, devices // group, permute_and_mix, 0)
    ping[pl.ds(devices, group)] = ping[pl.ds(0, group)]
    now, later = ping, pong
    for r in range(1, ROUNDS):
        off = jnp.left_shift(jnp.int32(1), shift_ref[r])

        def mix(n, _, now=now, later=later, off=off):
            for part in range(wide // group):
                base = n * wide + part * group
                back = (base - off) & mask
                later[pl.ds(base, group)] = (
                    now[pl.ds(base, group)] + now[pl.ds(back, group)]
                ) * 0.5
            return 0

        with jax.named_scope('s5_mix'):
            lax.fori_loop(0, devices // wide, mix, 0)
        if r < ROUNDS - 1:
            later[pl.ds(devices, group)] = later[pl.ds(0, group)]
        now, later = later, now
    done = now

    my_rows = pl.ds(pl.multiple_of(core * TILE[0], TILE[0]), TILE[0])
    my_lanes = pl.ds(pl.multiple_of(((y * count_x + x) * nx + gx) * TILE[1], TILE[1]), TILE[1])

    corner = [(0, 0), (0, 1), (0, count_x - 1), (1, 0), (count_y - 1, 0)][:5]
    corner = sorted(set(corner))
    planes = min(4, nx)
    early = len(corner) * planes * cores

    def give_to(there_y, there_x, there_gx, there_core):
        target = device_at(there_y, there_x, there_gx, there_core)
        worker = (target[0] * ny + target[1]) * nz + target[2]
        pltpu.make_async_remote_copy(
            src_ref=done.at[worker],
            dst_ref=mixed_ref.at[my_rows, my_lanes],
            send_sem=send_sem2,
            recv_sem=recv_sem2,
            device_id=target,
            device_id_type=MESH,
        ).start()

    def give_early(n, _):
        turn = lax.rem(n + me, early)
        there_core, there_gx = lax.rem(turn, cores), lax.rem(turn // cores, planes)
        column = turn // (cores * planes)
        there_y = there_x = jnp.int32(0)
        for c, (cy, cx) in enumerate(corner):
            there_y = jnp.where(column == c, cy, there_y)
            there_x = jnp.where(column == c, cx, there_x)
        myself = (there_y == y) & (there_x == x) & (there_gx == gx) & (there_core == core)

        @pl.when(jnp.logical_not(myself))
        def _():
            give_to(there_y, there_x, there_gx, there_core)

        return 0

    def give(step, _):
        there_y, there_x = column_at(columns - 1 - step)
        near = functools.reduce(
            jnp.logical_or, [(there_y == cy) & (there_x == cx) for cy, cx in corner]
        )
        for dx in reversed(zigzag(nx)):
            there_gx = lax.rem(gx + dx, nx)
            for dc in range(cores):
                there_core = lax.rem(core + dc, 2)
                skip = near & (there_gx < planes)
                if dx == 0 and dc == 0:
                    skip = skip | (step == columns - 1)

                @pl.when(jnp.logical_not(skip))
                def _():
                    give_to(there_y, there_x, there_gx, there_core)

        return 0

    with jax.named_scope("s6_give"):
        lax.fori_loop(0, early, give_early, 0)
        lax.fori_loop(0, columns, give, 0)
    mixed_ref[my_rows, my_lanes] = done[me]

    with jax.named_scope('s7_send1'):
        all_of(arrived, send_sem).wait()
    with jax.named_scope('s8_send2'):
        all_of(arrived, send_sem2).wait()
    with jax.named_scope('s9_recv2'):
        all_of(arrived, recv_sem2).wait()


def put_kernel(*refs):
    count = (len(refs) - 1) // 2
    sources, targets, sems = refs[:count], refs[count : 2 * count], refs[-1]
    parts = sems.shape[1]
    copies = []
    for n in range(count):
        width = sources[n].shape[1] // parts
        for p in range(parts):
            at = pl.ds(p * width, width)
            copies.append(
                pltpu.make_async_copy(sources[n].at[:, at], targets[n].at[:, at], sems.at[n, p])
            )
    for copy in copies:
        copy.start()
    for copy in copies:
        copy.wait()


def put(*arrays):
    parts = 4
    held = [pltpu.with_memory_space_constraint(a, pltpu.VMEM) for a in arrays]
    return pl.pallas_call(
        put_kernel,
        out_shape=[pltpu.HBM(a.shape, a.dtype) for a in arrays],
        in_specs=[pl.BlockSpec(memory_space=pltpu.VMEM)] * len(arrays),
        out_specs=[pl.BlockSpec(memory_space=pltpu.HBM)] * len(arrays),
        scratch_shapes=[pltpu.SemaphoreType.DMA((len(arrays), parts))],
        name="put",
    )(*held)


def shards(sizes, hidden_acts, output_grad, weights, momentum, worker_of_slot, round_shift):
    nx, ny, nz = sizes
    devices = nx * ny * nz
    hidden = hidden_acts.reshape(hidden_acts.shape[-2:])
    grad_out = output_grad.reshape(output_grad.shape[-2:]).T
    weight = weights.reshape(weights.shape[-2:])
    moment = momentum.reshape(momentum.shape[-2:])
    rows, width = weight.shape
    columns = devices // (2 * nx)
    tiles = (devices,) + TILE
    padded = (devices + 8,) + TILE
    inputs = [
        pltpu.with_memory_space_constraint(a, pltpu.HBM)
        for a in (grad_out, hidden, weight, moment, worker_of_slot.reshape(1, -1), round_shift)
    ]
    vmem, hbm = (pl.BlockSpec(memory_space=m) for m in (pltpu.VMEM, pltpu.HBM))
    mixed, new_moment = pl.pallas_call(
        functools.partial(kernel, sizes),
        out_shape=[pltpu.VMEM((rows, width), jnp.bfloat16)] * 2,
        in_specs=[hbm] * len(inputs),
        out_specs=[vmem, vmem],
        scratch_shapes=[
            pltpu.VMEM(hidden.shape, jnp.bfloat16),
            pltpu.VMEM((rows, width), jnp.bfloat16),
            pltpu.VMEM((rows, width), jnp.bfloat16),
            pltpu.VMEM(tiles, jnp.bfloat16),
            pltpu.VMEM(tiles, jnp.bfloat16),
            pltpu.VMEM(padded, jnp.bfloat16),
            pltpu.VMEM(padded, jnp.bfloat16),
            pltpu.VMEM((1, devices), jnp.int32),
            pltpu.SMEM((1, devices), jnp.int32),
            pltpu.VMEM(grad_out.shape, jnp.bfloat16),
            pltpu.VMEM((1, devices), jnp.int32),
            pltpu.SMEM((ROUNDS,), jnp.int32),
            pltpu.SemaphoreType.REGULAR((columns,)),
            pltpu.SemaphoreType.DMA((3, columns)),
            pltpu.SemaphoreType.DMA,
            pltpu.SemaphoreType.DMA((3,)),
            pltpu.SemaphoreType.DMA,
            pltpu.SemaphoreType.DMA,
            pltpu.SemaphoreType.DMA,
            pltpu.SemaphoreType.DMA,
        ],
        compiler_params=pltpu.CompilerParams(
            collective_id=0, has_side_effects=True, vmem_limit_bytes=40 * 1024 * 1024
        ),
        name="step",
    )(*inputs)
    mixed, new_moment = put(mixed, new_moment)
    return mixed.reshape(weights.shape), new_moment.reshape(momentum.shape)


def solution(mesh):
    sizes = tuple(mesh.shape[a] for a in ("gx", "gy", "gz"))
    placed = (
        P("gz", "gy", "gx", None, None),
        P("gz", "gy", "gx", None, None),
        P("gz", "gy", "gx", None, None),
        P("gz", "gy", "gx", None, None),
        P(),
        P(),
    )
    return jax.shard_map(
        functools.partial(shards, sizes),
        mesh=mesh,
        in_specs=placed,
        out_specs=(P("gx", "gy", "gz", None, None), P("gz", "gy", "gx", None, None)),
        check_vma=False,
    )
```

```python
import functools

import jax
import jax.numpy as jnp
from jax import lax
from jax.experimental import pallas as pl
from jax.experimental.pallas import tpu as pltpu
from jax.sharding import PartitionSpec as P

ROUNDS = 8
learn_rate = 0.01
beta_keep = 0.9
MESH = pl.DeviceIdType.MESH
TILE = (16, 128)


def zigzag(count):
    order = [0]
    for step in range(1, count // 2 + 1):
        order += sorted({step, count - step})
    return order


def kernel(
    sizes, grad_hbm, hidden_hbm, weight_hbm, moment_hbm, held_hbm, shift_hbm,
    mixed_ref, moment_out,
    hidden, weight, moment, outgoing, arrived, ping, pong, table, source_ref,
    grad_ref, held_ref, shift_ref, ready, in_sems, table_sem, small_sems, send_sem, recv_sem, send_sem2, recv_sem2,
):
    nx, ny, nz = sizes
    devices = nx * ny * nz
    gx, gy, gz = (lax.axis_index(a) for a in ("gx", "gy", "gz"))
    me = (gx * ny + gy) * nz + gz
    cores, low_x = 2, nz // 2
    count_y, count_x = ny // 2, 2 * low_x
    core = lax.rem(gz, 2)
    x = lax.rem(gy, 2) * low_x + gz // 2
    y = gy // 2
    columns = count_x * count_y
    chunk = nx * TILE[1]

    def spread(turn):
        along_y = turn * count_x
        along_x = turn - (count_y - 1)
        rest = turn - (count_y + count_x - 1)
        others = (1 + rest // (count_x - 1)) * count_x + 1 + lax.rem(rest, count_x - 1)
        return jnp.where(
            turn < count_y, along_y, jnp.where(turn < count_y + count_x - 1, along_x, others)
        )

    def column_at(step):
        there_y = lax.rem(y + step // count_x, count_y)
        there_x = lax.rem(x + lax.rem(step, count_x), count_x)
        return there_y, there_x

    def device_at(there_y, there_x, there_gx, there_core):
        there_gy = there_y * 2 + there_x // low_x
        there_gz = lax.rem(there_x, low_x) * 2 + there_core
        return there_gx, there_gy, there_gz

    barrier = pltpu.get_barrier_semaphore()

    def tell(semaphore, target):
        pl.semaphore_signal(semaphore, inc=1, device_id=target, device_id_type=MESH)

    def peer(dy, dx):
        return device_at(lax.rem(y + dy, count_y), lax.rem(x + dx, count_x), gx, core)

    def greet():
        for dx in zigzag(nx):
            for dc in range(cores):
                if dx or dc:
                    tell(barrier, device_at(y, x, lax.rem(gx + dx, nx), lax.rem(core + dc, 2)))
        for dy in range(1, count_y):
            tell(barrier, peer(dy, 0))
        for dx in range(1, count_x):
            tell(barrier, peer(0, dx))

    def vouch_to(dy, dx, about_y):
        seen_y = (count_y - dy + about_y) % count_y
        tell(ready.at[seen_y * count_x + (count_x - dx) % count_x], peer(dy, dx))

    def meet():
        pl.semaphore_wait(barrier, nx * cores - 1 + count_y - 1 + count_x - 1)
        for dy in range(1, count_y):
            vouch_to(dy, 0, 0)
        for dx in range(1, count_x):
            vouch_to(0, dx, 0)

    def await_column(step):
        pl.semaphore_wait(ready.at[step], 1)
        for dy in range(1, count_y):

            @pl.when(step == dy * count_x)
            def _():
                for dx in range(1, count_x):
                    vouch_to(0, dx, dy)

    def loads(step):
        there_y, there_x = column_at(step)
        at = pl.ds(pl.multiple_of((there_y * count_x + there_x) * chunk, chunk), chunk)
        return [
            pltpu.make_async_copy(big.at[:, at], small.at[:, at], in_sems.at[n, step])
            for n, (big, small) in enumerate(
                ((hidden_hbm, hidden), (weight_hbm, weight), (moment_hbm, moment))
            )
        ]

    def start_load(turn, _):
        for copy in loads(spread(turn)):
            copy.start()
        return 0

    small_loads = [
        pltpu.make_async_copy(far, near, small_sems.at[n])
        for n, (far, near) in enumerate(
            ((grad_hbm, grad_ref), (held_hbm, held_ref), (shift_hbm, shift_ref))
        )
    ]
    for copy in small_loads:
        copy.start()
    with jax.named_scope("s1_greet"):
        greet()
        lax.fori_loop(0, columns, start_load, 0)

    def tile_of(there_y, there_x, there_gx, there_core):
        return ((there_y * count_x + there_x) * nx + there_gx) * 2 + there_core

    my_tile = tile_of(y, x, gx, core)
    for copy in small_loads:
        copy.wait()
    grad_out = grad_ref[...]

    def send_tiles(step, there_core):
        there_y, there_x = column_at(step)
        for dx in zigzag(nx):
            there_gx = lax.rem(gx + dx, nx)
            target = device_at(there_y, there_x, there_gx, there_core)

            def send():
                pltpu.make_async_remote_copy(
                    src_ref=outgoing.at[tile_of(there_y, there_x, there_gx, there_core)],
                    dst_ref=arrived.at[me],
                    send_sem=send_sem,
                    recv_sem=recv_sem,
                    device_id=target,
                    device_id_type=MESH,
                ).start()

            if dx == 0:
                pl.when((step > 0) | (core != there_core))(send)
            else:
                send()

    def compute(turn, _):
        step = spread(turn)
        there_y, there_x = column_at(step)
        base = pl.multiple_of((there_y * count_x + there_x) * chunk, chunk)
        at = pl.ds(base, chunk)
        for copy in loads(step):
            copy.wait()
        grad = jnp.dot(grad_out, hidden[:, at], preferred_element_type=jnp.float32)
        velocity = beta_keep * moment[:, at].astype(jnp.float32) + grad
        moment_out[:, at] = velocity.astype(jnp.bfloat16)
        stepped = (weight[:, at].astype(jnp.float32) - learn_rate * velocity).astype(jnp.bfloat16)
        first = (there_y * count_x + there_x) * nx * 2
        for n in range(nx):
            for c in range(cores):
                outgoing[first + n * 2 + c] = stepped[
                    c * TILE[0] : (c + 1) * TILE[0], n * TILE[1] : (n + 1) * TILE[1]
                ]

        @pl.when(step > 0)
        def _():
            await_column(step)

        send_tiles(step, 0)
        return 0

    with jax.named_scope("s2_barrier"):
        meet()
    with jax.named_scope('s2_compute'):
        lax.fori_loop(0, columns, compute, 0)

    def second_wave(step, _):
        send_tiles(step, 1)
        return 0

    with jax.named_scope('s2_wave'):
        lax.fori_loop(0, columns, second_wave, 0)
    arrived[me] = outgoing[my_tile]

    held = jnp.broadcast_to(held_ref[...], (8, devices)).T[:, :1]
    slot = lax.broadcasted_iota(jnp.int32, (devices, devices), 0)
    worker = lax.broadcasted_iota(jnp.int32, (devices, devices), 1)
    place = (lax.rem(slot, nx) * ny + lax.rem(slot // nx, ny)) * nz + slot // (nx * ny)
    table[...] = jnp.sum(jnp.where(held == worker, place, 0), axis=0, keepdims=True) & (devices - 1)
    to_scalars = pltpu.make_async_copy(table, source_ref, table_sem)
    to_scalars.start()
    to_scalars.wait()

    def all_of(ref, sem):
        piece = ref.at[pl.ds(0, devices - 1)]
        return pltpu.make_async_copy(piece, piece, sem)

    with jax.named_scope('s3_recv1'):
        all_of(arrived, recv_sem).wait()

    group = 8
    wide = 16
    mask = devices - 1
    first_off = jnp.left_shift(jnp.int32(1), shift_ref[0])

    def permute_and_mix(n, _):
        base = n * group
        for t in range(group):
            k = base + t
            one = arrived[source_ref[0, k]]
            two = arrived[source_ref[0, (k - first_off) & mask]]
            ping[k] = (one + two) * 0.5
        return 0

    with jax.named_scope('s4_perm'):
        lax.fori_loop(0, devices // group, permute_and_mix, 0)
    ping[pl.ds(devices, group)] = ping[pl.ds(0, group)]
    now, later = ping, pong
    for r in range(1, ROUNDS):
        off = jnp.left_shift(jnp.int32(1), shift_ref[r])

        def mix(n, _, now=now, later=later, off=off):
            for part in range(wide // group):
                base = n * wide + part * group
                back = (base - off) & mask
                later[pl.ds(base, group)] = (
                    now[pl.ds(base, group)] + now[pl.ds(back, group)]
                ) * 0.5
            return 0

        with jax.named_scope('s5_mix'):
            lax.fori_loop(0, devices // wide, mix, 0)
        if r < ROUNDS - 1:
            later[pl.ds(devices, group)] = later[pl.ds(0, group)]
        now, later = later, now
    done = now

    my_rows = pl.ds(pl.multiple_of(core * TILE[0], TILE[0]), TILE[0])
    my_lanes = pl.ds(pl.multiple_of(((y * count_x + x) * nx + gx) * TILE[1], TILE[1]), TILE[1])

    corner = [(0, 0), (0, 1), (0, count_x - 1), (1, 0), (count_y - 1, 0)]
    corner = sorted(set(corner))
    planes = min(4, nx)
    early = len(corner) * planes * cores
    portions = min(4, columns)

    def give_to(there_y, there_x, there_gx, there_core):
        target = device_at(there_y, there_x, there_gx, there_core)
        worker = (target[0] * ny + target[1]) * nz + target[2]
        pltpu.make_async_remote_copy(
            src_ref=done.at[worker],
            dst_ref=mixed_ref.at[my_rows, my_lanes],
            send_sem=send_sem2,
            recv_sem=recv_sem2,
            device_id=target,
            device_id_type=MESH,
        ).start()

    def give_early(n, _):
        turn = lax.rem(n + me, early)
        there_core, there_gx = lax.rem(turn, cores), lax.rem(turn // cores, planes)
        column = turn // (cores * planes)
        there_y = there_x = jnp.int32(0)
        for c, (cy, cx) in enumerate(corner):
            there_y = jnp.where(column == c, cy, there_y)
            there_x = jnp.where(column == c, cx, there_x)
        myself = (there_y == y) & (there_x == x) & (there_gx == gx) & (there_core == core)

        @pl.when(jnp.logical_not(myself))
        def _():
            give_to(there_y, there_x, there_gx, there_core)

        return 0

    def give(step, _):
        size = jnp.where(core == 0, -(-early // columns), -(-early // portions))
        start, stop = (jnp.minimum(n * size, early) for n in (step, step + 1))
        lax.fori_loop(start, stop, give_early, 0)
        there_y, there_x = column_at(columns - 1 - step)
        near = functools.reduce(
            jnp.logical_or, [(there_y == cy) & (there_x == cx) for cy, cx in corner]
        )
        for dx in reversed(zigzag(nx)):
            there_gx = lax.rem(gx + dx, nx)
            for dc in range(cores):
                there_core = lax.rem(core + dc, 2)
                skip = near & (there_gx < planes)
                if dx == 0 and dc == 0:
                    skip = skip | (step == columns - 1)

                @pl.when(jnp.logical_not(skip))
                def _():
                    give_to(there_y, there_x, there_gx, there_core)

        return 0

    with jax.named_scope("s6_give"):
        lax.fori_loop(0, columns, give, 0)
    mixed_ref[my_rows, my_lanes] = done[me]

    with jax.named_scope('s7_send1'):
        all_of(arrived, send_sem).wait()
    with jax.named_scope('s8_send2'):
        all_of(arrived, send_sem2).wait()
    with jax.named_scope('s9_recv2'):
        all_of(arrived, recv_sem2).wait()


def put_kernel(*refs):
    count = (len(refs) - 1) // 2
    sources, targets, sems = refs[:count], refs[count : 2 * count], refs[-1]
    parts = sems.shape[1]
    copies = []
    for n in range(count):
        width = sources[n].shape[1] // parts
        for p in range(parts):
            at = pl.ds(p * width, width)
            copies.append(
                pltpu.make_async_copy(sources[n].at[:, at], targets[n].at[:, at], sems.at[n, p])
            )
    for copy in copies:
        copy.start()
    for copy in copies:
        copy.wait()


def put(*arrays):
    parts = 4
    held = [pltpu.with_memory_space_constraint(a, pltpu.VMEM) for a in arrays]
    return pl.pallas_call(
        put_kernel,
        out_shape=[pltpu.HBM(a.shape, a.dtype) for a in arrays],
        in_specs=[pl.BlockSpec(memory_space=pltpu.VMEM)] * len(arrays),
        out_specs=[pl.BlockSpec(memory_space=pltpu.HBM)] * len(arrays),
        scratch_shapes=[pltpu.SemaphoreType.DMA((len(arrays), parts))],
        name="put",
    )(*held)


def shards(sizes, hidden_acts, output_grad, weights, momentum, worker_of_slot, round_shift):
    nx, ny, nz = sizes
    devices = nx * ny * nz
    hidden = hidden_acts.reshape(hidden_acts.shape[-2:])
    grad_out = output_grad.reshape(output_grad.shape[-2:]).T
    weight = weights.reshape(weights.shape[-2:])
    moment = momentum.reshape(momentum.shape[-2:])
    rows, width = weight.shape
    columns = devices // (2 * nx)
    tiles = (devices,) + TILE
    padded = (devices + 8,) + TILE
    inputs = [
        pltpu.with_memory_space_constraint(a, pltpu.HBM)
        for a in (grad_out, hidden, weight, moment, worker_of_slot.reshape(1, -1), round_shift)
    ]
    vmem, hbm = (pl.BlockSpec(memory_space=m) for m in (pltpu.VMEM, pltpu.HBM))
    mixed, new_moment = pl.pallas_call(
        functools.partial(kernel, sizes),
        out_shape=[pltpu.VMEM((rows, width), jnp.bfloat16)] * 2,
        in_specs=[hbm] * len(inputs),
        out_specs=[vmem, vmem],
        scratch_shapes=[
            pltpu.VMEM(hidden.shape, jnp.bfloat16),
            pltpu.VMEM((rows, width), jnp.bfloat16),
            pltpu.VMEM((rows, width), jnp.bfloat16),
            pltpu.VMEM(tiles, jnp.bfloat16),
            pltpu.VMEM(tiles, jnp.bfloat16),
            pltpu.VMEM(padded, jnp.bfloat16),
            pltpu.VMEM(padded, jnp.bfloat16),
            pltpu.VMEM((1, devices), jnp.int32),
            pltpu.SMEM((1, devices), jnp.int32),
            pltpu.VMEM(grad_out.shape, jnp.bfloat16),
            pltpu.VMEM((1, devices), jnp.int32),
            pltpu.SMEM((ROUNDS,), jnp.int32),
            pltpu.SemaphoreType.REGULAR((columns,)),
            pltpu.SemaphoreType.DMA((3, columns)),
            pltpu.SemaphoreType.DMA,
            pltpu.SemaphoreType.DMA((3,)),
            pltpu.SemaphoreType.DMA,
            pltpu.SemaphoreType.DMA,
            pltpu.SemaphoreType.DMA,
            pltpu.SemaphoreType.DMA,
        ],
        compiler_params=pltpu.CompilerParams(
            collective_id=0, has_side_effects=True, vmem_limit_bytes=40 * 1024 * 1024
        ),
        name="step",
    )(*inputs)
    mixed, new_moment = put(mixed, new_moment)
    return mixed.reshape(weights.shape), new_moment.reshape(momentum.shape)


def solution(mesh):
    sizes = tuple(mesh.shape[a] for a in ("gx", "gy", "gz"))
    placed = (
        P("gz", "gy", "gx", None, None),
        P("gz", "gy", "gx", None, None),
        P("gz", "gy", "gx", None, None),
        P("gz", "gy", "gx", None, None),
        P(),
        P(),
    )
    return jax.shard_map(
        functools.partial(shards, sizes),
        mesh=mesh,
        in_specs=placed,
        out_specs=(P("gx", "gy", "gz", None, None), P("gz", "gy", "gx", None, None)),
        check_vma=False,
    )
```
